256 devices in a mesh: row: 8 (over x, y_hi), col: 32 (over z, y_lo, core).
Axes of the slice: x: 4, y: 4 (y_hi: 2, y_lo: 2; y = y_hi * 2 + y_lo), z: 8, core: 2. Of those that a mesh axis runs over, the one named last changes fastest.
Arguments:
- grams: bfloat16 [4, 8, 32, 32, 8192], P(None, None, 'col', None, 'row'), may hold values from -2.6 to 32, as said below
- adjusted: bfloat16 [4, 8192, 1024], P(None, ('row', 'col')), may hold values from -6 to 6
Outputs:
- merged: float32 [8192, 1024], P(('row', 'col'))
- residual_norms: float32 [3], replicated
The draws below stay inside these ranges and needn't reach their ends.
Inputs may be any that keep to these rules, and one draw needn't show every extreme that they name: `grams`: each G_m is symmetric positive definite.
All inputs are finite; a program needn't handle non-finite values.
Results may differ from the reference program's by a relative error of at most 0.0041.
Values may be sent and summed in bfloat16 or wider, within the bound.
A program may use at most 64 MiB of HBM per device.

```python
import jax
import jax.numpy as jnp
from jax import lax

D = 8192
OUT = 1024
MODELS = 4
SWEEPS = 3
BLOCK = 32
N_ROW = 8
N_COL = 32


def noise_field(noise_key):
    noise = jnp.clip(jax.random.normal(noise_key, (D, D), jnp.float32), -4.0, 4.0)
    return (noise + noise.T) * (0.7071068 / jnp.sqrt(jnp.float32(D)))


def draw_grams(key, part):
    base = jax.random.fold_in(key, 17)
    shared_key, scale_key, order_key, member_root = jax.random.split(base, 4)
    shared = 0.95 * noise_field(shared_key)
    offsets = jax.random.uniform(scale_key, (MODELS,), jnp.float32, 0.0, 1.0)
    order = jax.random.permutation(order_key, MODELS).astype(jnp.float32)
    scales = jnp.exp(2.0794415 * (order + offsets) / MODELS)
    keys = jax.random.split(member_root, MODELS)
    eye = jnp.eye(D, dtype=jnp.float32)

    def one_gram(inputs):
        member_key, scale = inputs
        noise_key, diag_key = jax.random.split(member_key)
        coupling = (shared + 0.3 * noise_field(noise_key)) * (1.0 - eye)
        diagonal = 2.5 * jnp.exp(jax.random.uniform(diag_key, (D,), jnp.float32, 0.0, 0.47000363))
        return scale * (coupling + eye * diagonal[None, :])
    gram = lax.map(one_gram, (keys, scales))
    return gram.reshape(MODELS, D // (N_COL * BLOCK), N_COL, BLOCK, D).astype(jnp.bfloat16)


def block_scale(stream_key, extent, pieces, least, top_value):
    factor_of, own = 1.0, jax.random.fold_in(stream_key, 6)
    for dim, parts in pieces:
        steps = jnp.exp(jax.random.uniform(jax.random.fold_in(own, dim), (parts,), jnp.float32, least / len(pieces), top_value / len(pieces)))
        factor_of = factor_of * jnp.repeat(steps, extent[dim] // parts).reshape([-1 if axis == dim else 1 for axis in range(len(extent))])
    return factor_of


def gaussian(key, shape, deviation, bound, shards=(), kind=jnp.bfloat16):
    gain = block_scale(key, shape, shards, -0.22, 0.18) if shards else 1.0
    array = jax.random.normal(key, shape, jnp.float32) * deviation * gain
    return jnp.minimum(jnp.maximum(array, -bound), bound).astype(kind)


def setup_inputs(seed: int = 0) -> dict:
    streams_of = jax.random.split(jax.random.key(seed), 3)
    return {
        "grams": draw_grams(jax.random.fold_in(streams_of[2], 71), 0),
        "adjusted": gaussian(streams_of[1], (MODELS, D, OUT), 1.0, 6.0, ((1, 256),)),
    }


SHRINK = 0.9

def block_solve(factor, rows):
    lower = lax.linalg.triangular_solve(factor, rows, left_side=True, lower=True)
    return lax.linalg.triangular_solve(factor, lower, left_side=True, lower=True, transpose_a=True)

def reference(grams, adjusted):
    gram = grams.reshape(MODELS, D, D)
    total32 = jnp.zeros((D, D), jnp.float32)
    rhs_gram = jnp.zeros((D, OUT), jnp.float32)
    for member in range(MODELS):
        total32 = total32 + gram[member].astype(jnp.float32)
        rhs_gram = rhs_gram + jnp.dot(gram[member].astype(jnp.float32), adjusted[member].astype(jnp.float32), preferred_element_type=jnp.float32)
    diag_each = jnp.diagonal(gram, axis1=1, axis2=2).astype(jnp.float32)
    diag_sum = lax.optimization_barrier(jnp.sum(diag_each, 0))
    gram_total = total32.astype(jnp.bfloat16)
    weights32 = adjusted.astype(jnp.float32)
    rhs = SHRINK * rhs_gram + (1.0 - SHRINK) * lax.optimization_barrier(jnp.sum(diag_each[:, :, None] * weights32, 0))
    blocks_count = N_ROW * N_COL
    index = jnp.arange(blocks_count)
    blocks = total32.reshape(blocks_count, BLOCK, blocks_count, BLOCK)[index, :, index, :]
    precond = SHRINK * blocks + (1.0 - SHRINK) * jax.vmap(jnp.diag)(diag_sum.reshape(blocks_count, BLOCK))
    factor = jnp.linalg.cholesky(precond)
    merged = lax.optimization_barrier(jnp.mean(weights32, 0))
    squares = []
    for sweep_index in range(SWEEPS):
        image = SHRINK * jnp.dot(gram_total.astype(jnp.float32), merged.astype(jnp.bfloat16).astype(jnp.float32), preferred_element_type=jnp.float32)
        image = image + (1.0 - SHRINK) * diag_sum[:, None] * merged
        resid = rhs - image
        squares.append(jnp.sum(resid * resid))
        update = block_solve(factor, resid.reshape(blocks_count, BLOCK, OUT))
        merged = merged + update.reshape(D, OUT)
    norms = jnp.sqrt(jnp.stack(squares) / jnp.sum(rhs * rhs))
    return (merged, norms)
```

```python
import jax
import jax.numpy as jnp
from jax import lax
from jax.experimental import pallas as pl
from jax.experimental.pallas import tpu as pltpu
from jax.sharding import Mesh
from jax.sharding import PartitionSpec as P

SWEEPS = 3
COL = ("z", "yl", "core")
ROW = ("x", "yh")
ROW_COL = ROW + COL
NX, NYH, NZ, NYL, NC = 4, 2, 8, 2, 2
NR = NX * NYH
BLK = 32
SUB = 2 * BLK
HALF = 256
CH = 128
SHRINK = 0.9
REST = 1.0 - SHRINK
F32, BF16 = jnp.float32, jnp.bfloat16
MESH_ID = pl.DeviceIdType.MESH
N_AG = 22
HI = lax.Precision.HIGHEST


def kernel(
    g_hbm, w_hbm, out_hbm, norm_ref,
    gbuf, tot, wbuf, mbuf, acc_r, acc_i, m0s, sendb, recvb, pinv, mst, outst, nb_a, nb_b, nb_c,
    ag_s, ag_r, rs_s, rs_r, in_s, in_r, in_l, out_s, out_r, out_l, n_s, n_r,
):
    x, yh = lax.axis_index("x"), lax.axis_index("yh")
    z, yl, core = lax.axis_index("z"), lax.axis_index("yl"), lax.axis_index("core")
    r = x * NYH + yh
    pairs = 1 - core
    rows = gbuf.shape[2]

    def at_z(d):
        return lax.rem(z + d + NZ, NZ)

    def row_peer(j):
        return {"x": lax.rem(x + j // 2, NX), "yh": (yh + j % 2) % 2}

    def rest_peer(e):
        return {"yl": (yl + e // 2) % 2, "core": (core + e % 2) % 2}

    def remote(src, dst, ss, rs, dev):
        return pltpu.make_async_remote_copy(
            src_ref=src, dst_ref=dst, send_sem=ss, recv_sem=rs, device_id=dev, device_id_type=MESH_ID
        )

    barrier = pltpu.get_barrier_semaphore()
    peers = [row_peer(j) for j in range(1, NR)]
    peers += [{"z": at_z(d)} for d in range(1, NZ)]
    peers += [rest_peer(e) for e in range(1, 4)]
    for dev in peers:
        pl.semaphore_signal(barrier, inc=1, device_id=dev, device_id_type=MESH_ID)

    own0 = wbuf.at[z, yl]
    local = []
    for n in range(2):
        lanes = pl.ds(pl.multiple_of(core * 512 + n * HALF, HALF), HALF)
        local.append(
            pltpu.make_async_copy(
                w_hbm.at[:, :, lanes],
                own0.at[n, :, pl.ds(pl.multiple_of(core * BLK, BLK), BLK)],
                in_l.at[n],
            )
        )
    g_local = pltpu.make_async_copy(g_hbm, gbuf.at[core], in_l.at[2])
    for c in local:
        c.start()
    g_local.start()
    pl.semaphore_wait(barrier, len(peers))

    waits = []
    other = {"core": pairs}
    w_in = []
    for n in range(2):
        lanes = pl.ds(pl.multiple_of(pairs * 512 + n * HALF, HALF), HALF)
        dst = own0.at[n, :, pl.ds(pl.multiple_of(core * BLK, BLK), BLK)]
        c = remote(w_hbm.at[:, :, lanes], dst, in_s.at[n], in_r.at[n], other)
        c.start()
        waits.append(c)
        got = own0.at[n, :, pl.ds(pl.multiple_of(pairs * BLK, BLK), BLK)]
        w_in.append(remote(got, got, in_s.at[n], in_r.at[n], other))
    g_out = remote(g_hbm, gbuf.at[core], in_s.at[2], in_r.at[2], other)
    g_out.start()
    waits.append(g_out)
    for c in local:
        c.wait()
    for c in w_in:
        c.wait_recv()

    def gather(buf, s, step):
        count = [0]

        def send(ref, i, dev):
            c = remote(ref, ref, ag_s.at[s, count[0]], ag_r.at[s, i], dev)
            count[0] += 1
            c.start()
            waits.append(c)

        def arrived(ref, i):
            remote(ref, ref, ag_s.at[s, 0], ag_r.at[s, i], {"yl": 1 - yl}).wait_recv()

        up, down, side = {"z": at_z(1)}, {"z": at_z(-1)}, {"yl": 1 - yl}
        own = buf.at[z, yl]
        send(own, 0, up)
        send(own, 4, down)
        send(own, 7, side)
        for h in range(1, 5):
            ref = buf.at[at_z(-h), yl]
            arrived(ref, h - 1)
            if h <= 3:
                send(ref, h, up)
            send(ref.at[1], 15 + h - 1, side)
            if h <= 3:
                ref = buf.at[at_z(h), yl]
                arrived(ref, 4 + h - 1)
                if h <= 2:
                    send(ref, 4 + h, down)
                send(ref.at[1], 19 + h - 1, side)
            d = h - 1
            if d == 0:
                ref = buf.at[z, 1 - yl]
                arrived(ref, 7)
                send(ref.at[0], 8, up)
                send(ref.at[0], 11, down)
                step([z], True)
            else:
                ref = buf.at[at_z(-d), 1 - yl, 0]
                arrived(ref, 8 + d - 1)
                if d <= 2:
                    send(ref, 8 + d, up)
                ref = buf.at[at_z(d), 1 - yl, 0]
                arrived(ref, 11 + d - 1)
                send(ref, 11 + d, down)
                arrived(buf.at[at_z(-d), 1 - yl, 1], 15 + d - 1)
                arrived(buf.at[at_z(d), 1 - yl, 1], 19 + d - 1)
                step([at_z(-d), at_z(d)], False)
        arrived(buf.at[at_z(4), 1 - yl, 0], 14)
        arrived(buf.at[at_z(4), 1 - yl, 1], 18)
        step([at_z(4)], False)

    def scatter(i, value):
        for j in range(1, NR):
            dev = row_peer(j)
            a = dev["x"] * NYH + dev["yh"]
            for n in range(2):
                sendb[i, a, n] = value(a, n).astype(BF16)
            c = remote(sendb.at[i, a], recvb.at[i, j], rs_s.at[i, j], rs_r.at[i, j], dev)
            c.start()
            waits.append(c)

    def reduced(i, value):
        total = [value(r, n) for n in range(2)]
        for j in range(1, NR):
            ref = recvb.at[i, j]
            remote(ref, ref, rs_s.at[i, j], rs_r.at[i, j], row_peer(1)).wait_recv()
            total = [total[n] + recvb[i, j, n].astype(F32) for n in range(2)]
        return total

    def take(acc_ref):
        def value(a, n):
            lines = pl.ds(pl.multiple_of(a * BLK, BLK), BLK)
            return jnp.concatenate([acc_ref[k, n, lines, :] for k in range(2)], axis=0)
        return value

    def prepare():
        g_local.wait()
        remote(gbuf.at[pairs], gbuf.at[pairs], in_s.at[2], in_r.at[2], other).wait_recv()
        acc_r[...] = jnp.zeros_like(acc_r)
        acc_i[...] = jnp.zeros_like(acc_i)

        def sum_rows(i, carry):
            k, lines = i // 8, pl.ds(pl.multiple_of(lax.rem(i, 8) * BLK, BLK), BLK)
            value = gbuf[k, 0, lines, :].astype(F32)
            for m in range(1, 4):
                value = value + gbuf[k, m, lines, :].astype(F32)
            tot[k, lines, :] = value.astype(BF16)
            return carry

        lax.fori_loop(0, 16, sum_rows, 0)

    def columns(zz):
        return pl.ds(pl.multiple_of(zz * CH, CH), CH)

    def first_step(chunks, start):
        if start:
            prepare()
        for zz in chunks:
            def per_half(n, carry):
                rowsw = [wbuf[zz, :, n, m].reshape(CH, HALF) for m in range(4)]
                mean = (
                    rowsw[0].astype(F32) + rowsw[1].astype(F32) + rowsw[2].astype(F32) + rowsw[3].astype(F32)
                ) * 0.25
                m0s[...] = mean.astype(BF16)

                def per_tile(k, carry):
                    value = acc_r[k, n]
                    for m in range(4):
                        value = value + jnp.dot(
                            gbuf[k, m, :, columns(zz)], wbuf[zz, :, n, m].reshape(CH, HALF),
                            preferred_element_type=F32,
                        )
                    acc_r[k, n] = value
                    acc_i[0, k, n] = acc_i[0, k, n] + jnp.dot(
                        tot[k, :, columns(zz)], m0s[...], preferred_element_type=F32
                    )
                    return carry

                return lax.fori_loop(0, 2, per_tile, carry)

            lax.fori_loop(0, 2, per_half, 0)

    def sweep_step(s):
        def step(chunks, start):
            for zz in chunks:
                def per(i, carry):
                    k, n = i // 2, lax.rem(i, 2)
                    acc_i[s, k, n] = acc_i[s, k, n] + jnp.dot(
                        tot[k, :, columns(zz)], mbuf[s - 1, zz, :, n].reshape(CH, HALF),
                        preferred_element_type=F32,
                    )
                    return carry

                lax.fori_loop(0, 4, per, 0)
        return step

    gather(wbuf, 0, first_step)

    take_r = take(acc_r)
    take_i = [take(acc_i.at[s]) for s in range(SWEEPS)]

    def first_value(a, n):
        return take_r(a, n) - take_i[0](a, n)

    scatter(0, first_value)

    lane = lax.broadcasted_iota(jnp.int32, (2, BLK, CH), 2)
    line = lax.broadcasted_iota(jnp.int32, (2, BLK, CH), 1)
    tile = lax.broadcasted_iota(jnp.int32, (2, BLK, CH), 0)
    at = lane - yl * SUB - tile * BLK
    inside = (at >= 0) & (at < BLK)
    lines = pl.ds(pl.multiple_of(r * BLK, BLK), BLK)
    diag_each, block = [], None
    for m in range(4):
        part = jnp.stack([gbuf[k, m, lines, columns(z)] for k in range(2)], axis=0).astype(F32)
        diag_each.append(jnp.sum(jnp.where(at == line, part, 0.0), axis=2, keepdims=True))
        block = part if block is None else block + part
    diag_sum = diag_each[0] + diag_each[1] + diag_each[2] + diag_each[3]
    matrix = jnp.where(inside, SHRINK * block, 0.0) + jnp.where(at == line, REST * diag_sum, 0.0)

    def eliminate(j, mat):
        row = jnp.sum(jnp.where(line == j, mat, 0.0), axis=1, keepdims=True)
        col = jnp.sum(jnp.where(at == j, mat, 0.0), axis=2, keepdims=True)
        piv = jnp.sum(jnp.where(at[:, :1, :] == j, row, 0.0), axis=2, keepdims=True)
        inv = 1.0 / piv
        scaled = row * inv
        new = jnp.where(at == j, 0.0, mat) - col * jnp.where(at[:, :1, :] == j, inv, scaled)
        return jnp.where(line == j, jnp.where(at == j, inv, scaled), new)

    pinv[...] = lax.fori_loop(0, BLK, eliminate, matrix).reshape(SUB, CH)

    diag64 = diag_sum.reshape(SUB, 1)
    own = [wbuf[z, yl, n] for n in range(2)]
    merged, rest = [], []
    for n in range(2):
        w32 = [own[n][m].astype(F32) for m in range(4)]
        merged.append((w32[0] + w32[1] + w32[2] + w32[3]) * 0.25)
        rest.append(sum(diag_each[m].reshape(SUB, 1) * w32[m] for m in range(4)) * REST)

    def solve(resid):
        return jnp.dot(
            pinv[...], jnp.concatenate([resid, resid], axis=0), precision=HI, preferred_element_type=F32
        )

    def squares(parts):
        return jnp.sum(parts[0] * parts[0]) + jnp.sum(parts[1] * parts[1])

    got = reduced(0, first_value)
    resid = [SHRINK * got[n] + rest[n] - REST * diag64 * merged[n] for n in range(2)]
    sums = [squares(resid)]
    for s in range(1, SWEEPS):
        update = [solve(resid[n]) for n in range(2)]
        for n in range(2):
            merged[n] = merged[n] + update[n]
            mbuf[s - 1, z, yl, n] = merged[n].astype(BF16)
        gather(mbuf.at[s - 1], s, sweep_step(s))

        def change(a, n):
            return take_i[s](a, n) - take_i[s - 1](a, n)

        scatter(s, change)
        if s == 1:
            scatter(3, take_r)
        else:
            rhs = reduced(3, take_r)
            sums_rhs = squares([SHRINK * rhs[n] + rest[n] for n in range(2)])
        got = reduced(s, change)
        resid = [resid[n] - SHRINK * got[n] - REST * diag64 * update[n] for n in range(2)]
        sums.append(squares(resid))
    sums.append(sums_rhs)

    index = lax.broadcasted_iota(jnp.int32, (8, 128), 0)
    value = jnp.zeros((8, 128), F32)
    for i in range(4):
        value = jnp.where(index == i, sums[i], value)
    nb_a[r] = value
    for j in range(1, NR):
        c = remote(nb_a.at[r], nb_a.at[r], n_s.at[0, j], n_r.at[0, j], row_peer(j))
        c.start()
        waits.append(c)

    for n in range(2):
        mst[n] = merged[n] + solve(resid[n])
    final = []
    for n in range(2):
        lanes = pl.ds(pl.multiple_of(core * 512 + n * HALF, HALF), HALF)
        src = mst.at[n, pl.ds(pl.multiple_of(pairs * BLK, BLK), BLK)]
        c = remote(src, outst.at[:, lanes], out_s.at[n], out_r.at[n], other)
        c.start()
        waits.append(c)
        src = mst.at[n, pl.ds(pl.multiple_of(core * BLK, BLK), BLK)]
        c = pltpu.make_async_copy(src, out_hbm.at[:, lanes], out_l.at[n])
        c.start()
        final.append(c)
    for n in range(2):
        lanes = pl.ds(pl.multiple_of(pairs * 512 + n * HALF, HALF), HALF)
        remote(outst.at[:, lanes], outst.at[:, lanes], out_s.at[n], out_r.at[n], other).wait_recv()
        c = pltpu.make_async_copy(outst.at[:, lanes], out_hbm.at[:, lanes], out_l.at[2 + n])
        c.start()
        final.append(c)

    def summed(nb, stage, count, index_of, peer_of):
        for j in range(1, count):
            ref = nb.at[index_of(j)]
            remote(ref, ref, n_s.at[stage, j], n_r.at[stage, j], peer_of(1)).wait_recv()
        value = nb[0]
        for j in range(1, count):
            value = value + nb[j]
        return value

    def row_from(j):
        return lax.rem(x + NX - j // 2, NX) * NYH + (yh + j % 2) % 2

    nb_b[z] = summed(nb_a, 0, NR, row_from, row_peer)
    for d in range(1, NZ):
        c = remote(nb_b.at[z], nb_b.at[z], n_s.at[1, d], n_r.at[1, d], {"z": at_z(d)})
        c.start()
        waits.append(c)
    place = yl * 2 + core
    nb_c[place] = summed(nb_b, 1, NZ, lambda d: at_z(-d), lambda d: {"z": at_z(d)})
    for e in range(1, 4):
        c = remote(nb_c.at[place], nb_c.at[place], n_s.at[2, e], n_r.at[2, e], rest_peer(e))
        c.start()
        waits.append(c)

    def rest_from(e):
        return ((yl + e // 2) % 2) * 2 + (core + e % 2) % 2

    totals = summed(nb_c, 2, 4, rest_from, rest_peer)
    norm_ref[...] = jnp.sqrt(totals / totals[3:4, :])
    for c in final:
        c.wait()
    for c in waits:
        c.wait_send()


def local(grams, adjusted):
    models, major, _, sub_rows, columns = grams.shape
    outs = adjusted.shape[2]
    g = grams.reshape(models, major * sub_rows, columns)
    rows = major * sub_rows
    dma = pltpu.SemaphoreType.DMA
    vmem = pltpu.VMEM
    merged, norms = pl.pallas_call(
        kernel,
        out_shape=(
            jax.ShapeDtypeStruct((sub_rows, outs), F32),
            jax.ShapeDtypeStruct((8, 128), F32),
        ),
        in_specs=[pl.BlockSpec(memory_space=pl.ANY)] * 2,
        out_specs=(pl.BlockSpec(memory_space=pl.ANY), pl.BlockSpec(memory_space=pltpu.VMEM)),
        scratch_shapes=[
            vmem((2, models, rows, columns), BF16),
            vmem((2, rows, columns), BF16),
            vmem((NZ, 2, 2, models, SUB, HALF), BF16),
            vmem((2, NZ, 2, 2, SUB, HALF), BF16),
            vmem((2, 2, rows, HALF), F32),
            vmem((SWEEPS, 2, 2, rows, HALF), F32),
            vmem((CH, HALF), BF16),
            vmem((4, NR, 2, SUB, HALF), BF16),
            vmem((4, NR, 2, SUB, HALF), BF16),
            vmem((SUB, CH), F32),
            vmem((2, SUB, HALF), F32),
            vmem((sub_rows, outs), F32),
            vmem((NR, 8, 128), F32),
            vmem((NZ, 8, 128), F32),
            vmem((4, 8, 128), F32),
            dma((3, N_AG)),
            dma((3, N_AG)),
            dma((4, NR)),
            dma((4, NR)),
            dma((3,)),
            dma((3,)),
            dma((3,)),
            dma((2,)),
            dma((2,)),
            dma((4,)),
            dma((3, NR)),
            dma((3, NR)),
        ],
        compiler_params=pltpu.CompilerParams(
            collective_id=0, has_side_effects=True, vmem_limit_bytes=48 * 1024 * 1024
        ),
        name="merge",
    )(g, adjusted)
    return merged, norms[:SWEEPS, 0]


def solution(mesh):
    finer = Mesh(mesh.devices.reshape(NX, NYH, NZ, NYL, NC), ROW_COL)
    placed = (P(None, None, COL, None, ROW), P(None, ROW_COL, None))
    return jax.shard_map(
        local, mesh=finer, in_specs=placed, out_specs=(P(ROW_COL, None), P()), check_vma=False
    )
```
